32 devices in a mesh: fsdp: 16 (over z, y, x), mat: 2 (over core).
Axes of the slice: x: 2, y: 2, z: 4, core: 2. Of those that a mesh axis runs over, the one named last changes fastest.
Arguments:
- momentum: float32 [8192, 4096], P(('mat', 'fsdp')), parts along dimension 0, may hold values from -6 to 6
- grad: bfloat16 [8192, 4096], P(('mat', 'fsdp')), parts along dimension 0, may hold values from -6 to 6
- q_basis: float32 [8192, 512], P(('mat', 'fsdp')), parts along dimension 0, may hold values from -6 to 6
Outputs:
- momentum_next: float32 [8192, 4096], P(('mat', 'fsdp')), parts along dimension 0
- update: bfloat16 [8192, 4096], P(('mat', 'fsdp')), parts along dimension 0
- q_next: float32 [8192, 512], P(('mat', 'fsdp')), parts along dimension 0
The draws below stay inside these ranges and needn't reach their ends.
There are 2 independent parts, one for each index of `mat`. The reference program is written for one: setup_inputs(seed, part) draws one part's arguments, and reference() takes and returns one part's arrays. A program takes and returns all parts, laid end to end along the dimension named above; each array names one. Nothing has to cross between parts.
All inputs are finite; a program needn't handle non-finite values.
Results may differ from the reference program's by a relative error of at most 0.0076.
Values may be sent and summed in bfloat16 or wider, within the bound.
A program may use at most 128 MiB of HBM per device.

```python
import math
import jax
import jax.numpy as jnp
from jax import lax

D = 4096
RANK = 512
ROWS = 4096


def with_spikes(drawn, stream_key, source, target, parts, factor):
    def block_of(axis_at):
        return (jnp.arange(drawn.shape[axis_at]) // (drawn.shape[axis_at] // parts)).reshape((-1,) + (1,) * (drawn.ndim - 1 - axis_at))

    first = jax.random.permutation(stream_key, parts)[block_of(target)]
    other_side = (block_of(target) + parts // 2) % parts
    return jnp.where((block_of(source) == first) | (block_of(source) == other_side), factor * drawn, drawn)


def block_levels(key, extent, split, least, high):
    loudness, own = 1.0, jax.random.fold_in(key, 6)
    for dim, shards_of in split:
        heights = jnp.exp(jax.random.uniform(jax.random.fold_in(own, dim), (shards_of,), jnp.float32, least / len(split), high / len(split)))
        loudness = loudness * jnp.repeat(heights, extent[dim] // shards_of).reshape([-1 if axis == dim else 1 for axis in range(len(extent))])
    return loudness


def bell_draw(own_key, shape, deviation, limit, shards=(), kind=jnp.bfloat16):
    entries = jax.random.normal(own_key, shape, jnp.float32) * deviation
    if len(shards) > 0:
        entries = block_levels(own_key, shape, shards, -0.22, 0.18) * entries
    return jnp.clip(entries, min=-limit, max=limit).astype(kind)


def heavy_noise(stream_key, dims, deviation, bound, pieces, heavy, kind=jnp.bfloat16):
    drawn = deviation * jax.random.normal(stream_key, dims, jnp.float32)
    if pieces:
        drawn = drawn * block_levels(stream_key, dims, pieces, -0.22, 0.18)
    return jnp.clip(with_spikes(drawn, jax.random.fold_in(stream_key, 3), *heavy), -bound, bound).astype(kind)


def setup_inputs(seed: int = 0, part: int = 0) -> dict:
    keys = jax.random.split(jax.random.key(seed), 4)
    part_splits = jax.random.split(jax.random.fold_in(keys[3], part), 4)
    return {
        "momentum": bell_draw(part_splits[0], (ROWS, D), 1.0, 6.0, ((0, 16),), jnp.float32),
        "grad": heavy_noise(part_splits[1], (ROWS, D), 1.0, 6.0, ((0, 16),), (0, 1, 16, 2.0)),
        "q_basis": bell_draw(part_splits[2], (D, RANK), 1.0, 6.0, ((0, 16),), jnp.float32),
    }


damping = 0.95
epsilon = 1e-06

def lower_inverse(gram_total):
    order_size = gram_total.shape[0]
    identity = jnp.eye(order_size, dtype=jnp.float32)
    ridge_term = 0.0001 * jnp.trace(gram_total) / order_size
    factor_lower = jnp.linalg.cholesky(gram_total + ridge_term * identity)
    return lax.linalg.triangular_solve(factor_lower, identity, left_side=True, lower=True)

def reference(momentum, grad, q_basis):
    blended = momentum + grad.astype(jnp.float32)
    projected = jnp.dot(blended.astype(jnp.bfloat16).astype(jnp.float32), q_basis.astype(jnp.bfloat16).astype(jnp.float32), preferred_element_type=jnp.float32)
    gram_total = jnp.dot(projected.T, projected, precision=lax.Precision.HIGHEST)
    inverse = lower_inverse(gram_total)
    orthonormal = jnp.dot(projected, inverse.T, precision=lax.Precision.HIGHEST)
    summed = jnp.dot(blended.T, orthonormal, precision=lax.Precision.HIGHEST)
    column_rms = jnp.sqrt(lax.optimization_barrier(jnp.mean(summed * summed, axis=0)) + epsilon)
    q_next = summed / column_rms
    q_low = q_next.astype(jnp.bfloat16)
    error_low = (orthonormal * column_rms).astype(jnp.bfloat16)
    ortho_low = orthonormal.astype(jnp.bfloat16)
    error_term = jnp.dot(error_low.astype(jnp.float32), q_low.T.astype(jnp.float32), preferred_element_type=jnp.float32)
    step_term = jnp.dot(ortho_low.astype(jnp.float32), q_low.T.astype(jnp.float32), preferred_element_type=jnp.float32)
    momentum_next = blended - (1.0 - damping) * error_term
    update = (math.sqrt(ROWS * D / RANK) * step_term).astype(jnp.bfloat16)
    return (momentum_next, update, q_next)
```

```python
import functools
import math

import jax
import jax.numpy as jnp
from jax import lax
from jax.experimental import pallas as pl
from jax.experimental.pallas import tpu as pltpu
from jax.sharding import PartitionSpec as P

damping = 0.95
epsilon = 1e-06
HIGHEST = lax.Precision.HIGHEST
MESH = pl.DeviceIdType.MESH


def grid_of(mesh):
    n = mesh.shape["fsdp"]
    at = list(mesh.axis_names).index("fsdp")
    try:
        line = mesh.devices.swapaxes(0, at).reshape(n, -1)[:, 0]
        spots = [tuple(d.coords) for d in line]
        axes = []
        for d in range(3):
            size = len({s[d] for s in spots})
            if size > 1:
                stride = next(i for i in range(n) if spots[i][d] != spots[0][d])
                axes.append((stride, size))
        sizes = [size for _, size in sorted(axes, reverse=True)]
        if math.prod(sizes) == n:
            return tuple([1] * (3 - len(sizes)) + sizes)
    except AttributeError:
        pass
    return (n // 4, 2, 2) if n % 4 == 0 else (1, 1, n)


def cut(rows, unit, sizes):
    units = rows // unit
    side = (units * 3 + 4) // 8
    counts = [side, side, units - 2 * side]
    long_axis = max(range(3), key=lambda d: sizes[d])
    others = [d for d in range(3) if d != long_axis]
    orders = [
        (long_axis, others[0], others[1]),
        (others[1], long_axis, others[0]),
        (others[0], others[1], long_axis),
    ]
    pieces, start = [], 0
    for count, order in zip(counts, orders):
        if count:
            pieces.append((start, count * unit, order))
        start += count * unit
    return pieces


def position(sizes):
    me = lax.axis_index("fsdp")
    return [
        lax.div(me, sizes[1] * sizes[2]),
        lax.rem(lax.div(me, sizes[2]), sizes[1]),
        lax.rem(me, sizes[2]),
    ]


def shifted(mine, sizes, d, off):
    return lax.rem(mine[d] + off, sizes[d])


def device_at(mine, sizes, d, coordinate):
    spot = list(mine)
    spot[d] = coordinate
    return {"fsdp": (spot[0] * sizes[1] + spot[1]) * sizes[2] + spot[2]}


def greet(mine, sizes):
    barrier = pltpu.get_barrier_semaphore()
    for d in range(3):
        for off in range(1, sizes[d]):
            target = device_at(mine, sizes, d, shifted(mine, sizes, d, off))
            pl.semaphore_signal(barrier, inc=1, device_id=target, device_id_type=MESH)
    pl.semaphore_wait(barrier, sum(sizes) - 3)


def gather_kernel(sizes, pieces, x_ref, o_ref, own_sem, send_sem, recv_sem):
    mine = position(sizes)
    own = pltpu.make_async_copy(x_ref, o_ref.at[mine[0], mine[1], mine[2]], own_sem)
    own.start()
    greet(mine, sizes)

    def block(piece, phase, coordinate):
        start, rows, order = piece
        index = list(mine)
        index[order[phase]] = coordinate
        for d in order[:phase]:
            index[d] = slice(None)
        return o_ref.at[index[0], index[1], index[2], pl.ds(start, rows)]

    sent = []
    for phase in range(3):
        if phase == 1:
            own.wait()
        for p, piece in enumerate(pieces):
            if phase:
                d = piece[2][phase - 1]
                for off in range(1, sizes[d]):
                    landed = block(piece, phase - 1, shifted(mine, sizes, d, sizes[d] - off))
                    pltpu.make_async_copy(landed, landed, recv_sem.at[p, phase - 1, off]).wait()
            d = piece[2][phase]
            for off in range(1, sizes[d]):
                target = block(piece, phase, mine[d])
                source = x_ref.at[pl.ds(piece[0], piece[1])] if phase == 0 else target
                copy = pltpu.make_async_remote_copy(
                    src_ref=source,
                    dst_ref=target,
                    send_sem=send_sem.at[p, phase, off],
                    recv_sem=recv_sem.at[p, phase, off],
                    device_id=device_at(mine, sizes, d, shifted(mine, sizes, d, off)),
                    device_id_type=MESH,
                )
                copy.start()
                sent.append(copy)
    for p, piece in enumerate(pieces):
        d = piece[2][2]
        for off in range(1, sizes[d]):
            landed = block(piece, 2, shifted(mine, sizes, d, sizes[d] - off))
            pltpu.make_async_copy(landed, landed, recv_sem.at[p, 2, off]).wait()
    for copy in sent:
        copy.wait_send()


def gather(x, sizes, number):
    rows, columns = x.shape
    unit = 8 if x.dtype == jnp.float32 else 16
    pieces = cut(rows, unit, sizes)
    sems = pltpu.SemaphoreType.DMA((len(pieces), 3, max(sizes)))
    out = pl.pallas_call(
        functools.partial(gather_kernel, sizes, pieces),
        out_shape=jax.ShapeDtypeStruct(sizes + (rows, columns), x.dtype),
        in_specs=[pl.BlockSpec(memory_space=pltpu.VMEM)],
        out_specs=pl.BlockSpec(memory_space=pltpu.VMEM),
        scratch_shapes=[pltpu.SemaphoreType.DMA, sems, sems],
        compiler_params=pltpu.CompilerParams(
            collective_id=number, has_side_effects=True, vmem_limit_bytes=32 * 2**20
        ),
        name=f"gather_{number}",
    )(x)
    return out.reshape(math.prod(sizes) * rows, columns)


def reduce_kernel(sizes, pieces, x_ref, o_ref, *scratch):
    mine = position(sizes)
    count = len(pieces)
    landing = scratch[: 3 * count]
    sums = scratch[3 * count : 5 * count]
    send_sem, recv_sem = scratch[5 * count :]
    greet(mine, sizes)
    sent = []

    def send(p, phase, d, off, source):
        copy = pltpu.make_async_remote_copy(
            src_ref=source,
            dst_ref=landing[3 * p + phase].at[off - 1],
            send_sem=send_sem.at[p, phase, off],
            recv_sem=recv_sem.at[p, phase, off],
            device_id=device_at(mine, sizes, d, shifted(mine, sizes, d, off)),
            device_id_type=MESH,
        )
        copy.start()
        sent.append(copy)

    def arrive(p, phase, d):
        for off in range(1, sizes[d]):
            here = landing[3 * p + phase].at[off - 1]
            pltpu.make_async_copy(here, here, recv_sem.at[p, phase, off]).wait()

    for p, (start, rows, order) in enumerate(pieces):
        d = order[2]
        for off in range(1, sizes[d]):
            index = [slice(None)] * 3
            index[d] = shifted(mine, sizes, d, off)
            send(p, 0, d, off, x_ref.at[index[0], index[1], index[2], pl.ds(start, rows)])

    for p, (start, rows, order) in enumerate(pieces):
        a, b, c = order
        arrive(p, 0, c)
        low, high = min(a, b), max(a, b)
        for off in list(range(1, sizes[b])) + [0]:
            at_b = shifted(mine, sizes, b, off)

            def one(at_a, _, off=off, at_b=at_b):
                index = [None] * 3
                index[a], index[b], index[c] = at_a, at_b, mine[c]
                total = x_ref[index[0], index[1], index[2], pl.ds(start, rows)].astype(jnp.float32)
                for k in range(sizes[c] - 1):
                    total += landing[3 * p][k, index[low], index[high]].astype(jnp.float32)
                if off:
                    sums[2 * p][off - 1, at_a] = total.astype(x_ref.dtype)
                else:
                    sums[2 * p + 1][at_a] = total
                return 0

            lax.fori_loop(0, sizes[a], one, 0)
        for off in range(1, sizes[b]):
            send(p, 1, b, off, sums[2 * p].at[off - 1])

    for p, (start, rows, order) in enumerate(pieces):
        a, b, c = order
        arrive(p, 1, b)
        for off in list(range(1, sizes[a])) + [0]:
            at_a = shifted(mine, sizes, a, off)
            total = sums[2 * p + 1][at_a]
            for k in range(sizes[b] - 1):
                total += landing[3 * p + 1][k, at_a].astype(jnp.float32)
            if off:
                landing[3 * p + 2][sizes[a] - 1 + off - 1] = total.astype(x_ref.dtype)
            else:
                sums[2 * p + 1][at_a] = total
        for off in range(1, sizes[a]):
            send(p, 2, a, off, landing[3 * p + 2].at[sizes[a] - 1 + off - 1])

    for p, (start, rows, order) in enumerate(pieces):
        a = order[0]
        arrive(p, 2, a)
        total = sums[2 * p + 1][mine[a]]
        for k in range(sizes[a] - 1):
            total += landing[3 * p + 2][k].astype(jnp.float32)
        o_ref[pl.ds(start, rows)] = total
    for copy in sent:
        copy.wait_send()


def reduce_scatter(x, sizes, number):
    n = math.prod(sizes)
    rows, columns = x.shape[0] // n, x.shape[1]
    unit = 8 if x.dtype == jnp.float32 else 16
    pieces = cut(rows, unit, sizes)
    landing, sums = [], []
    for _, part, (a, b, c) in pieces:
        low, high = min(a, b), max(a, b)
        many = lambda k: max(k, 1)
        landing += [
            pltpu.VMEM((many(sizes[c] - 1), sizes[low], sizes[high], part, columns), x.dtype),
            pltpu.VMEM((many(sizes[b] - 1), sizes[a], part, columns), x.dtype),
            pltpu.VMEM((many(2 * (sizes[a] - 1)), part, columns), x.dtype),
        ]
        sums += [
            pltpu.VMEM((many(sizes[b] - 1), sizes[a], part, columns), x.dtype),
            pltpu.VMEM((sizes[a], part, columns), jnp.float32),
        ]
    sems = pltpu.SemaphoreType.DMA((len(pieces), 3, max(sizes)))
    return pl.pallas_call(
        functools.partial(reduce_kernel, sizes, pieces),
        out_shape=jax.ShapeDtypeStruct((rows, columns), jnp.float32),
        in_specs=[pl.BlockSpec(memory_space=pltpu.VMEM)],
        out_specs=pl.BlockSpec(memory_space=pltpu.VMEM),
        scratch_shapes=landing + sums + [sems, sems],
        compiler_params=pltpu.CompilerParams(
            collective_id=number, has_side_effects=True, vmem_limit_bytes=40 * 2**20
        ),
        name=f"reduce_{number}",
    )(x.reshape(sizes + (rows, columns)))


def dot_first(left, right):
    return lax.dot_general(
        left, right, (((0,), (0,)), ((), ())), precision=HIGHEST, preferred_element_type=jnp.float32
    )


def inverse_kernel(size, width, g_ref, x_ref, a_ref, d_ref):
    eye = lax.broadcasted_iota(jnp.int32, (size, size), 0) == lax.broadcasted_iota(
        jnp.int32, (size, size), 1
    )
    gram = g_ref[...]
    trace = jnp.sum(jnp.where(eye, gram, 0.0), keepdims=True)
    a_ref[...] = gram + jnp.where(eye, 0.0001 * trace / size, 0.0)
    x_ref[...] = jnp.where(eye, 1.0, 0.0)
    strip = lax.broadcasted_iota(jnp.int32, (8, width), 0)
    lane = lax.broadcasted_iota(jnp.int32, (8, width), 1)
    small_eye = jnp.where(
        lax.broadcasted_iota(jnp.int32, (width, width), 0)
        == lax.broadcasted_iota(jnp.int32, (width, width), 1),
        1.0,
        0.0,
    )

    def group(g, _):
        first = pl.multiple_of(g * 8, 8)
        left = d_ref[pl.ds(first, 8), :width]
        right = d_ref[pl.ds(first, 8), width:]
        turned = pltpu.roll(left, lax.rem(width - first, width), 1)
        columns = [jnp.broadcast_to(turned[:, j : j + 1], (8, width)) for j in range(8)]
        for j in range(8):
            scale = lax.rsqrt(columns[j][j : j + 1, :])
            factor = columns[j] * scale
            for m in range(j + 1, 8):
                columns[m] = columns[m] - factor * factor[m : m + 1, :]
            row_left, row_right = left[j : j + 1, :] * scale, right[j : j + 1, :] * scale
            below, here = strip > j, strip == j
            left = jnp.where(here, row_left, jnp.where(below, left - factor * row_left, left))
            right = jnp.where(here, row_right, jnp.where(below, right - factor * row_right, right))
        later = jnp.where(lane >= first + 8, left, 0.0)
        both = jnp.concatenate([left, right], axis=1)
        d_ref[pl.ds(first, 8), :] = both
        d_ref[...] = d_ref[...] - dot_first(later, both)
        return 0

    for k in range(size // width):
        top, end = k * width, (k + 1) * width
        d_ref[:, :width] = a_ref[top:end, top:end]
        d_ref[:, width:] = small_eye
        lax.fori_loop(0, width // 8, group, 0)
        corner = d_ref[:, width:]
        done = jnp.dot(corner, x_ref[top:end, :end], precision=HIGHEST)
        x_ref[top:end, :end] = done
        if end < size:
            panel = jnp.dot(corner, a_ref[top:end, end:], precision=HIGHEST)
            a_ref[end:, end:] = a_ref[end:, end:] - dot_first(panel, panel)
            x_ref[end:, :end] = x_ref[end:, :end] - dot_first(panel, done)


def lower_inverse(gram_total):
    size = gram_total.shape[0]
    width = 128
    return pl.pallas_call(
        functools.partial(inverse_kernel, size, width),
        out_shape=jax.ShapeDtypeStruct((size, size), jnp.float32),
        in_specs=[pl.BlockSpec(memory_space=pltpu.VMEM)],
        out_specs=pl.BlockSpec(memory_space=pltpu.VMEM),
        scratch_shapes=[
            pltpu.VMEM((size, size), jnp.float32),
            pltpu.VMEM((width, 2 * width), jnp.float32),
        ],
        compiler_params=pltpu.CompilerParams(vmem_limit_bytes=24 * 2**20),
        name="lower_inverse",
    )(gram_total)


def per_device(sizes, momentum, grad, q_basis):
    own_rows = momentum.shape[0]
    basis_rows, rank = q_basis.shape
    devices = math.prod(sizes)
    features = basis_rows * devices
    blended = momentum + grad.astype(jnp.float32)
    blended_low = blended.astype(jnp.bfloat16)
    basis = gather(q_basis.astype(jnp.bfloat16), sizes, 0)
    projected = jnp.dot(blended_low, basis, preferred_element_type=jnp.float32)
    local_gram = jnp.dot(projected.T, projected, precision=HIGHEST)
    gram_total = gather(reduce_scatter(local_gram, sizes, 1), sizes, 2)
    inverse = lower_inverse(gram_total)
    orthonormal = jnp.dot(projected, inverse.T, precision=HIGHEST)
    ortho_low = orthonormal.astype(jnp.bfloat16)
    terms = jnp.dot(blended_low.T, ortho_low, preferred_element_type=jnp.float32)
    summed = reduce_scatter(terms.astype(jnp.bfloat16), sizes, 3)
    summed_low = gather(summed.astype(jnp.bfloat16), sizes, 4)
    wide = summed_low.astype(jnp.float32)
    column_rms = jnp.sqrt(jnp.mean(wide * wide, axis=0) + epsilon)
    q_next = summed / column_rms
    stacked = jnp.concatenate(
        [ortho_low, (orthonormal / column_rms).astype(jnp.bfloat16)], axis=0
    )
    result = jnp.dot(stacked, summed_low.T, preferred_element_type=jnp.float32)
    total_rows = own_rows * devices
    momentum_next = blended - (1.0 - damping) * result[:own_rows]
    update = (math.sqrt(total_rows * features / rank) * result[own_rows:]).astype(jnp.bfloat16)
    return (momentum_next, update, q_next)


def solution(mesh):
    spec = P(("mat", "fsdp"), None)
    return jax.shard_map(
        functools.partial(per_device, grid_of(mesh)),
        mesh=mesh,
        in_specs=(spec, spec, spec),
        out_specs=(spec, spec, spec),
        check_vma=False,
    )
```

```python
import functools
import math

import jax
import jax.numpy as jnp
from jax import lax
from jax.experimental import pallas as pl
from jax.experimental.pallas import tpu as pltpu
from jax.sharding import PartitionSpec as P

damping = 0.95
epsilon = 1e-06
HIGHEST = lax.Precision.HIGHEST
MESH = pl.DeviceIdType.MESH


def grid_of(mesh):
    n = mesh.shape["fsdp"]
    at = list(mesh.axis_names).index("fsdp")
    try:
        line = mesh.devices.swapaxes(0, at).reshape(n, -1)[:, 0]
        spots = [tuple(d.coords) for d in line]
        axes = []
        for d in range(3):
            size = len({s[d] for s in spots})
            if size > 1:
                stride = next(i for i in range(n) if spots[i][d] != spots[0][d])
                axes.append((stride, size))
        sizes = [size for _, size in sorted(axes, reverse=True)]
        if math.prod(sizes) == n:
            return tuple([1] * (3 - len(sizes)) + sizes)
    except AttributeError:
        pass
    return (n // 4, 2, 2) if n % 4 == 0 else (1, 1, n)


def cut(rows, unit, sizes):
    units = rows // unit
    long_axis = max(range(3), key=lambda d: sizes[d])
    first, second = [d for d in range(3) if d != long_axis]
    tail = units // 8
    pairs = 2 if units >= 8 else 1
    share, extra = divmod(units - tail, 2 * pairs)
    plan = [(tail, (first, second, long_axis), 0)]
    for k in range(2 * pairs):
        short = (first, second) if k % 2 == 0 else (second, first)
        plan.append((share + (k < extra), (long_axis,) + short, k // 2))
    pieces, start = [], 0
    for count, order, wave in plan:
        if count:
            pieces.append((start, count * unit, order, wave))
        start += count * unit
    return pieces


def wavefront(pieces, phases):
    steps = [(piece[3] + phase, phase, p) for p, piece in enumerate(pieces) for phase in range(phases)]
    return [(phase, p) for _, phase, p in sorted(steps)]


def position(sizes):
    me = lax.axis_index("fsdp")
    return [
        lax.div(me, sizes[1] * sizes[2]),
        lax.rem(lax.div(me, sizes[2]), sizes[1]),
        lax.rem(me, sizes[2]),
    ]


def shifted(mine, sizes, d, off):
    return lax.rem(mine[d] + off, sizes[d])


def device_at(mine, sizes, d, coordinate):
    spot = list(mine)
    spot[d] = coordinate
    return {"fsdp": (spot[0] * sizes[1] + spot[1]) * sizes[2] + spot[2]}


def greet(mine, sizes):
    barrier = pltpu.get_barrier_semaphore()
    for d in range(3):
        for off in range(1, sizes[d]):
            target = device_at(mine, sizes, d, shifted(mine, sizes, d, off))
            pl.semaphore_signal(barrier, inc=1, device_id=target, device_id_type=MESH)
    pl.semaphore_wait(barrier, sum(sizes) - 3)


def gather_kernel(sizes, pieces, x_ref, o_ref, own_sem, send_sem, recv_sem):
    mine = position(sizes)
    own = pltpu.make_async_copy(x_ref, o_ref.at[mine[0], mine[1], mine[2]], own_sem)
    own.start()
    greet(mine, sizes)

    def block(piece, phase, coordinate):
        start, rows, order, _ = piece
        index = list(mine)
        index[order[phase]] = coordinate
        for d in order[:phase]:
            index[d] = slice(None)
        return o_ref.at[index[0], index[1], index[2], pl.ds(start, rows)]

    sent = []
    own_here = False
    for phase, p in wavefront(pieces, 3):
        piece = pieces[p]
        if phase:
            if not own_here:
                own.wait()
                own_here = True
            d = piece[2][phase - 1]
            for off in range(1, sizes[d]):
                landed = block(piece, phase - 1, shifted(mine, sizes, d, sizes[d] - off))
                pltpu.make_async_copy(landed, landed, recv_sem.at[p, phase - 1, off]).wait()
        d = piece[2][phase]
        for off in range(1, sizes[d]):
            target = block(piece, phase, mine[d])
            source = x_ref.at[pl.ds(piece[0], piece[1])] if phase == 0 else target
            copy = pltpu.make_async_remote_copy(
                src_ref=source,
                dst_ref=target,
                send_sem=send_sem.at[p, phase, off],
                recv_sem=recv_sem.at[p, phase, off],
                device_id=device_at(mine, sizes, d, shifted(mine, sizes, d, off)),
                device_id_type=MESH,
            )
            copy.start()
            sent.append(copy)
    for p, piece in enumerate(pieces):
        d = piece[2][2]
        for off in range(1, sizes[d]):
            landed = block(piece, 2, shifted(mine, sizes, d, sizes[d] - off))
            pltpu.make_async_copy(landed, landed, recv_sem.at[p, 2, off]).wait()
    for copy in sent:
        copy.wait_send()


def gather(x, sizes, number):
    rows, columns = x.shape
    unit = 8 if x.dtype == jnp.float32 else 16
    pieces = cut(rows, unit, sizes)
    sems = pltpu.SemaphoreType.DMA((len(pieces), 3, max(sizes)))
    out = pl.pallas_call(
        functools.partial(gather_kernel, sizes, pieces),
        out_shape=jax.ShapeDtypeStruct(sizes + (rows, columns), x.dtype),
        in_specs=[pl.BlockSpec(memory_space=pltpu.VMEM)],
        out_specs=pl.BlockSpec(memory_space=pltpu.VMEM),
        scratch_shapes=[pltpu.SemaphoreType.DMA, sems, sems],
        compiler_params=pltpu.CompilerParams(
            collective_id=number, has_side_effects=True, vmem_limit_bytes=32 * 2**20
        ),
        name=f"gather_{number}",
    )(x)
    return out.reshape(math.prod(sizes) * rows, columns)


def reduce_kernel(sizes, pieces, x_ref, o_ref, *scratch):
    mine = position(sizes)
    count = len(pieces)
    landing = scratch[: 3 * count]
    sums = scratch[3 * count : 5 * count]
    send_sem, recv_sem = scratch[5 * count :]
    greet(mine, sizes)
    sent = []

    def send(p, phase, d, off, source):
        copy = pltpu.make_async_remote_copy(
            src_ref=source,
            dst_ref=landing[3 * p + phase].at[off - 1],
            send_sem=send_sem.at[p, phase, off],
            recv_sem=recv_sem.at[p, phase, off],
            device_id=device_at(mine, sizes, d, shifted(mine, sizes, d, off)),
            device_id_type=MESH,
        )
        copy.start()
        sent.append(copy)

    def arrive(p, phase, d):
        for off in range(1, sizes[d]):
            here = landing[3 * p + phase].at[off - 1]
            pltpu.make_async_copy(here, here, recv_sem.at[p, phase, off]).wait()

    def begin(p, start, rows, order):
        d = order[2]
        for off in range(1, sizes[d]):
            index = [slice(None)] * 3
            index[d] = shifted(mine, sizes, d, off)
            send(p, 0, d, off, x_ref.at[index[0], index[1], index[2], pl.ds(start, rows)])

    def first_sums(p, start, rows, order):
        a, b, c = order
        arrive(p, 0, c)
        low, high = min(a, b), max(a, b)
        for off in list(range(1, sizes[b])) + [0]:
            at_b = shifted(mine, sizes, b, off)

            def one(at_a, _, off=off, at_b=at_b):
                index = [None] * 3
                index[a], index[b], index[c] = at_a, at_b, mine[c]
                total = x_ref[index[0], index[1], index[2], pl.ds(start, rows)].astype(jnp.float32)
                for k in range(sizes[c] - 1):
                    total += landing[3 * p][k, index[low], index[high]].astype(jnp.float32)
                if off:
                    sums[2 * p][off - 1, at_a] = total.astype(x_ref.dtype)
                else:
                    sums[2 * p + 1][at_a] = total
                return 0

            lax.fori_loop(0, sizes[a], one, 0)
        for off in range(1, sizes[b]):
            send(p, 1, b, off, sums[2 * p].at[off - 1])

    def second_sums(p, start, rows, order):
        a, b, c = order
        arrive(p, 1, b)
        for off in list(range(1, sizes[a])) + [0]:
            at_a = shifted(mine, sizes, a, off)
            total = sums[2 * p + 1][at_a]
            for k in range(sizes[b] - 1):
                total += landing[3 * p + 1][k, at_a].astype(jnp.float32)
            if off:
                landing[3 * p + 2][sizes[a] - 1 + off - 1] = total.astype(x_ref.dtype)
            else:
                sums[2 * p + 1][at_a] = total
        for off in range(1, sizes[a]):
            send(p, 2, a, off, landing[3 * p + 2].at[sizes[a] - 1 + off - 1])

    def last_sums(p, start, rows, order):
        a = order[0]
        arrive(p, 2, a)
        total = sums[2 * p + 1][mine[a]]
        for k in range(sizes[a] - 1):
            total += landing[3 * p + 2][k].astype(jnp.float32)
        o_ref[pl.ds(start, rows)] = total

    stages = (begin, first_sums, second_sums, last_sums)
    for phase, p in wavefront(pieces, 4):
        stages[phase](p, *pieces[p][:3])
    for copy in sent:
        copy.wait_send()


def reduce_scatter(x, sizes, number):
    n = math.prod(sizes)
    rows, columns = x.shape[0] // n, x.shape[1]
    unit = 8 if x.dtype == jnp.float32 else 16
    pieces = cut(rows, unit, sizes)
    landing, sums = [], []
    for _, part, (a, b, c), _ in pieces:
        low, high = min(a, b), max(a, b)
        many = lambda k: max(k, 1)
        landing += [
            pltpu.VMEM((many(sizes[c] - 1), sizes[low], sizes[high], part, columns), x.dtype),
            pltpu.VMEM((many(sizes[b] - 1), sizes[a], part, columns), x.dtype),
            pltpu.VMEM((many(2 * (sizes[a] - 1)), part, columns), x.dtype),
        ]
        sums += [
            pltpu.VMEM((many(sizes[b] - 1), sizes[a], part, columns), x.dtype),
            pltpu.VMEM((sizes[a], part, columns), jnp.float32),
        ]
    sems = pltpu.SemaphoreType.DMA((len(pieces), 3, max(sizes)))
    return pl.pallas_call(
        functools.partial(reduce_kernel, sizes, pieces),
        out_shape=jax.ShapeDtypeStruct((rows, columns), jnp.float32),
        in_specs=[pl.BlockSpec(memory_space=pltpu.VMEM)],
        out_specs=pl.BlockSpec(memory_space=pltpu.VMEM),
        scratch_shapes=landing + sums + [sems, sems],
        compiler_params=pltpu.CompilerParams(
            collective_id=number, has_side_effects=True, vmem_limit_bytes=40 * 2**20
        ),
        name=f"reduce_{number}",
    )(x.reshape(sizes + (rows, columns)))


def dot_first(left, right):
    return lax.dot_general(
        left, right, (((0,), (0,)), ((), ())), precision=HIGHEST, preferred_element_type=jnp.float32
    )


def three(x):
    high = x.astype(jnp.bfloat16).astype(jnp.float32)
    rest = x - high
    middle = rest.astype(jnp.bfloat16).astype(jnp.float32)
    return high, middle, rest - middle


def short_dot(left, right):
    h, m, l = three(left)
    lefts = jnp.concatenate([h, h, m, m, h, l], axis=0).astype(jnp.bfloat16)
    h, m, l = three(right)
    rights = jnp.concatenate([h, m, h, m, l, h], axis=0).astype(jnp.bfloat16)
    return lax.dot_general(
        lefts, rights, (((0,), (0,)), ((), ())), preferred_element_type=jnp.float32
    )


def inverse_kernel(size, width, g_ref, x_ref, a_ref, d_ref):
    eye = lax.broadcasted_iota(jnp.int32, (size, size), 0) == lax.broadcasted_iota(
        jnp.int32, (size, size), 1
    )
    gram = g_ref[...]
    trace = jnp.sum(jnp.where(eye, gram, 0.0), keepdims=True)
    a_ref[...] = gram + jnp.where(eye, 0.0001 * trace / size, 0.0)
    x_ref[...] = jnp.where(eye, 1.0, 0.0)
    strip = lax.broadcasted_iota(jnp.int32, (8, width), 0)
    lane = lax.broadcasted_iota(jnp.int32, (8, width), 1)
    small_eye = jnp.where(
        lax.broadcasted_iota(jnp.int32, (width, width), 0)
        == lax.broadcasted_iota(jnp.int32, (width, width), 1),
        1.0,
        0.0,
    )

    def group(g, _):
        first = pl.multiple_of(g * 8, 8)
        left = d_ref[pl.ds(first, 8), :width]
        right = d_ref[pl.ds(first, 8), width:]
        turned = pltpu.roll(left, lax.rem(width - first, width), 1)
        columns = [jnp.broadcast_to(turned[:, j : j + 1], (8, width)) for j in range(8)]
        for j in range(8):
            scale = lax.rsqrt(columns[j][j : j + 1, :])
            factor = columns[j] * scale
            for m in range(j + 1, 8):
                columns[m] = columns[m] - factor * factor[m : m + 1, :]
            row_left, row_right = left[j : j + 1, :] * scale, right[j : j + 1, :] * scale
            below, here = strip > j, strip == j
            left = jnp.where(here, row_left, jnp.where(below, left - factor * row_left, left))
            right = jnp.where(here, row_right, jnp.where(below, right - factor * row_right, right))
        later = jnp.where(lane >= first + 8, left, 0.0)
        both = jnp.concatenate([left, right], axis=1)
        d_ref[pl.ds(first, 8), :] = both
        d_ref[...] = d_ref[...] - short_dot(later, both)
        return 0

    for k in range(size // width):
        top, end = k * width, (k + 1) * width
        d_ref[:, :width] = a_ref[top:end, top:end]
        d_ref[:, width:] = small_eye
        lax.fori_loop(0, width // 8, group, 0)
        corner = d_ref[:, width:]
        done = jnp.dot(corner, x_ref[top:end, :end], precision=HIGHEST)
        x_ref[top:end, :end] = done
        if end < size:
            panel = jnp.dot(corner, a_ref[top:end, end:], precision=HIGHEST)
            a_ref[end:, end:] = a_ref[end:, end:] - dot_first(panel, panel)
            x_ref[end:, :end] = x_ref[end:, :end] - dot_first(panel, done)


def lower_inverse(gram_total):
    size = gram_total.shape[0]
    width = 128
    return pl.pallas_call(
        functools.partial(inverse_kernel, size, width),
        out_shape=jax.ShapeDtypeStruct((size, size), jnp.float32),
        in_specs=[pl.BlockSpec(memory_space=pltpu.VMEM)],
        out_specs=pl.BlockSpec(memory_space=pltpu.VMEM),
        scratch_shapes=[
            pltpu.VMEM((size, size), jnp.float32),
            pltpu.VMEM((width, 2 * width), jnp.float32),
        ],
        compiler_params=pltpu.CompilerParams(vmem_limit_bytes=24 * 2**20),
        name="lower_inverse",
    )(gram_total)


def per_device(sizes, momentum, grad, q_basis):
    own_rows = momentum.shape[0]
    basis_rows, rank = q_basis.shape
    devices = math.prod(sizes)
    features = basis_rows * devices
    blended = momentum + grad.astype(jnp.float32)
    blended_low = blended.astype(jnp.bfloat16)
    basis = gather(q_basis.astype(jnp.bfloat16), sizes, 0)
    projected = jnp.dot(blended_low, basis, preferred_element_type=jnp.float32)
    local_gram = jnp.dot(projected.T, projected, precision=HIGHEST)
    gram_total = gather(reduce_scatter(local_gram, sizes, 1), sizes, 2)
    inverse = lower_inverse(gram_total)
    orthonormal = jnp.dot(projected, inverse.T, precision=HIGHEST)
    ortho_low = orthonormal.astype(jnp.bfloat16)
    terms = jnp.dot(blended_low.T, ortho_low, preferred_element_type=jnp.float32)
    summed = reduce_scatter(terms.astype(jnp.bfloat16), sizes, 3)
    summed_low = gather(summed.astype(jnp.bfloat16), sizes, 4)
    wide = summed_low.astype(jnp.float32)
    column_rms = jnp.sqrt(jnp.mean(wide * wide, axis=0) + epsilon)
    q_next = summed / column_rms
    stacked = jnp.concatenate(
        [ortho_low, (orthonormal / column_rms).astype(jnp.bfloat16)], axis=0
    )
    result = jnp.dot(stacked, summed_low.T, preferred_element_type=jnp.float32)
    total_rows = own_rows * devices
    momentum_next = blended - (1.0 - damping) * result[:own_rows]
    update = (math.sqrt(total_rows * features / rank) * result[own_rows:]).astype(jnp.bfloat16)
    return (momentum_next, update, q_next)


def solution(mesh):
    spec = P(("mat", "fsdp"), None)
    return jax.shard_map(
        functools.partial(per_device, grid_of(mesh)),
        mesh=mesh,
        in_specs=(spec, spec, spec),
        out_specs=(spec, spec, spec),
        check_vma=False,
    )
```
